32 devices in a mesh: dp: 2 (over z, core), tp: 16 (over x, y).
Axes of the slice: x: 4, y: 4, z: 1, core: 2. Of those that a mesh axis runs over, the one named last changes fastest.
The devices are a block of a 4x4x8 slice.
Arguments:
- x: bfloat16 [4096, 12288], P(('dp', 'tp')), parts along dimension 0
- gain: bfloat16 [12288], replicated
- wq: bfloat16 [12288, 12288], P(None, 'tp')
- wk: bfloat16 [12288, 12288], P(None, 'tp')
- wv: bfloat16 [12288, 12288], P(None, 'tp')
- wo: bfloat16 [12288, 12288], P('tp')
Outputs:
- output: bfloat16 [4096, 12288], P(('dp', 'tp')), parts along dimension 0
There are 2 independent parts. The reference program is written for one: setup_inputs(seed, part) draws one part's arguments, and reference() takes and returns one part's arrays. A program takes and returns all parts, laid end to end along the dimension named above; an argument that names none is the same for every part.
All inputs are finite; a program needn't handle non-finite values.
Results may differ from the reference program's by a relative error of at most 0.012.
Values are sent between devices in bfloat16 or wider.
A program may use at most 768 MiB of HBM per device.

```python
import jax
import jax.numpy as jnp
from jax import lax

ROWS = 2048
D = 12288
HEADS = 96
KV_HEADS = 96
HEAD = 128
THETA = 10000


def setup_inputs(seed: int = 0, part: int = 0) -> dict:
    kx, kn, kq, kk, kv, ko = jax.random.split(jax.random.key(seed), 6)

    def weights(key, rows, columns):
        return jax.random.normal(key, (rows, columns), jnp.float32) * rows**-0.5

    drawn = {
        "x": jax.random.normal(jax.random.fold_in(kx, part), (ROWS, D), jnp.float32),
        "gain": 1 + 0.1 * jax.random.normal(kn, (D,), jnp.float32),
        "wq": 2 * weights(kq, D, HEADS * HEAD),
        "wk": 2 * weights(kk, D, KV_HEADS * HEAD),
        "wv": 4 * weights(kv, D, KV_HEADS * HEAD),
        "wo": weights(ko, HEADS * HEAD, D),
    }
    return {k: v.astype(jnp.bfloat16) for k, v in drawn.items()}


def normed(x, gain):
    wide = x.astype(jnp.float32)
    scale = lax.rsqrt(jnp.mean(wide * wide, -1, keepdims=True) + 1e-6)
    return (wide * scale * gain.astype(jnp.float32)).astype(jnp.bfloat16)


def turned(t, place, theta):
    half = t.shape[-1] // 2
    angle = place.astype(jnp.float32)[:, None] * theta ** (-jnp.arange(half, dtype=jnp.float32) / half)
    cos, sin = jnp.cos(angle)[:, None], jnp.sin(angle)[:, None]
    a, b = t[..., :half].astype(jnp.float32), t[..., half:].astype(jnp.float32)
    return jnp.concatenate([a * cos - b * sin, b * cos + a * sin], -1).astype(jnp.bfloat16)


def matmul(a, w):
    return jnp.dot(a, w, preferred_element_type=jnp.float32).astype(jnp.bfloat16)


def einsum(form, a, b):
    return jnp.einsum(form, a.astype(jnp.float32), b.astype(jnp.float32))


def attention(q, k, v):
    scores = einsum("tgsd,ugd->gstu", q, k) * q.shape[-1] ** -0.5
    token = jnp.arange(q.shape[0])
    scores = jnp.where(token[:, None] >= token, scores, -jnp.inf)
    weights = jax.nn.softmax(scores, -1).astype(jnp.bfloat16)
    return einsum("gstu,ugd->tgsd", weights, v).astype(jnp.bfloat16)


def reference(x, gain, wq, wk, wv, wo):
    a, place = normed(x, gain), jnp.arange(ROWS)
    q = turned(matmul(a, wq).reshape(ROWS, HEADS, HEAD), place, THETA).reshape(ROWS, KV_HEADS, -1, HEAD)
    k = turned(matmul(a, wk).reshape(ROWS, KV_HEADS, HEAD), place, THETA)
    v = matmul(a, wv).reshape(ROWS, KV_HEADS, HEAD)
    seen = attention(q, k, v).reshape(ROWS, HEADS * HEAD)
    return (x.astype(jnp.float32) + jnp.dot(seen, wo, preferred_element_type=jnp.float32)).astype(jnp.bfloat16)
```

```python
import functools

import jax
import jax.numpy as jnp
from jax import lax
from jax.experimental import pallas as pl
from jax.experimental.pallas import tpu as pltpu

NEG = -1e30
HIDDEN = 2 * NEG
LOG2E = 1.4426950408889634


def _dot(a, b, ca, cb):
    return lax.dot_general(a, b, (((ca,), (cb,)), ((), ())), preferred_element_type=jnp.float32)


import math

import numpy as np
from jax.sharding import PartitionSpec as P

HEAD = 128
THETA = 10000
RINGS = 4
CUTS = 4
FULL = 67043328
MESH_ID = pl.DeviceIdType.MESH


def _place(me, cycle, side):
    x, y = lax.div(me, side), lax.rem(me, side)
    return (y * side if cycle else x * side) + lax.rem(x + y, side)


def _device(place, cycle, side):
    place = lax.rem(place, side * side)
    i, k = lax.div(place, side), lax.rem(place, side)
    j = lax.rem(k - i + side, side)
    return j * side + i if cycle else i * side + j


def _ring(me, r, hops, side):
    n = side * side
    cycle, back = divmod(r, 2)
    return _device(_place(me, cycle, side) + (2 * n - hops if back else 2 * n + hops), cycle, side)


def _greet(me, side):
    barrier = pltpu.get_barrier_semaphore()
    for r in range(RINGS):
        pl.semaphore_signal(barrier, inc=1, device_id={"tp": _ring(me, r, 1, side)}, device_id_type=MESH_ID)
    return lambda: pl.semaphore_wait(barrier, RINGS)


def _gather_kernel(n, x_ref, gain_ref, cs_ref, wq_ref, wk_ref, wv_ref, all_ref, q_ref, k_ref, v_ref,
                   w_s, acc_s, a_s, o_s, cs_s, x_sem, w_sem, own_sem, send_sem, recv_sem, load_sem, cs_sem, out_sem):
    side = math.isqrt(n)
    me = lax.axis_index("tp")
    rows, depth = x_ref.shape
    part = rows // RINGS
    width = depth // CUTS
    one = wq_ref.shape[1]
    heads = one // HEAD
    ready = _greet(me, side)

    def columns(j):
        return pl.ds(pl.multiple_of(j * width, width), width)

    def home(j):
        return a_s.at[j // 2, pl.ds((j % 2) * rows, rows), :]

    for r in range(RINGS):
        for j in range(CUTS):
            pltpu.make_async_copy(x_ref.at[pl.ds(r * part, part), columns(j)], home(j).at[pl.ds(r * part, part), :], x_sem.at[r]).start()

    def remote(src, r, s, j):
        b = _ring(me, r, -s, side)
        at = pl.ds(pl.multiple_of(b * rows + r * part, part), part)
        src = all_ref.at[j, at, :] if src is None else src
        return pltpu.make_async_remote_copy(src_ref=src, dst_ref=all_ref.at[j, at, :], send_sem=send_sem.at[s, j], recv_sem=recv_sem.at[s + 1, j],
                                            device_id={"tp": _ring(me, r, 1, side)}, device_id_type=MESH_ID)

    for r in range(RINGS):
        pltpu.make_async_copy(a_s.at[0, pl.ds(0, CUTS * part), :], a_s.at[0, pl.ds(0, CUTS * part), :], x_sem.at[r]).wait()
        for g in range(0, part, 16):
            at = [(j // 2, (j % 2) * rows + r * part + g) for j in range(CUTS)]
            total = jnp.zeros((16, 1), jnp.float32)
            for c, t in at:
                wide = a_s[c, t : t + 16, :].astype(jnp.float32)
                total += jnp.sum(wide * wide, -1, keepdims=True)
            scale = lax.rsqrt(total / depth + 1e-6)
            for j, (c, t) in enumerate(at):
                wide = a_s[c, t : t + 16, :].astype(jnp.float32)
                a_s[c, t : t + 16, :] = (wide * scale * gain_ref[:, j * width : (j + 1) * width].astype(jnp.float32)).astype(jnp.bfloat16)
        if r == 0:
            ready()
        for j in range(CUTS):
            remote(home(j).at[pl.ds(r * part, part), :], r, 0, j).start()
    own = [pltpu.make_async_copy(home(j), all_ref.at[j, pl.ds(pl.multiple_of(me * rows, rows), rows), :], own_sem) for j in range(CUTS)]
    for c in own:
        c.start()
    for j in range(CUTS):
        for i, w in enumerate((wq_ref, wk_ref, wv_ref)):
            pltpu.make_async_copy(w.at[columns(j), :], w_s.at[columns(j), pl.ds(i * one, one)], w_sem.at[j]).start()
    acc_s[...] = jnp.zeros_like(acc_s)

    def sent(s, j):
        pltpu.make_async_copy(all_ref.at[0, pl.ds(0, rows), :], all_ref.at[0, pl.ds(0, rows), :], send_sem.at[s, j]).wait()

    def arrive(s, j, last):
        pltpu.make_async_copy(all_ref.at[0, pl.ds(0, rows), :], all_ref.at[0, pl.ds(0, rows), :], recv_sem.at[s, j]).wait()

        @pl.when(jnp.logical_not(last))
        def _():
            for r in range(RINGS):
                remote(None, r, s, j).start()

    pieces = [(u, r) for u in range(2) for r in range(RINGS)]

    def token(p, u, r):
        return pl.multiple_of(_ring(me, r, -(2 * p + u), side) * rows + r * part, part)

    def task(e):
        s = lax.div(e, CUTS) + 1
        return s, lax.rem(e, CUTS), lax.div(s - 1, 2), lax.rem(s, 2) == 1

    def written():
        pltpu.make_async_copy(o_s, o_s, out_sem).wait()

    def finish(p):
        pl.when(p > 0)(written)
        pltpu.make_async_copy(cs_s, cs_s, cs_sem).wait()
        step = 64
        for t in range(0, 2 * rows, step):
            cs = cs_s[t : t + step, :]
            sc = pltpu.roll(cs, HEAD // 2, 1)
            low = lax.broadcasted_iota(jnp.int32, cs.shape, 1) < HEAD // 2
            cos, sin = jnp.where(low, cs, sc), jnp.where(low, -sc, cs)
            for h in range(3 * heads):
                got = acc_s[t : t + step, h * HEAD : (h + 1) * HEAD]
                if h < 2 * heads:
                    got = got.astype(jnp.bfloat16).astype(jnp.float32)
                    got = got * cos + pltpu.roll(got, HEAD // 2, 1) * sin
                o_s[h // heads, h % heads, t : t + step, :] = got.astype(jnp.bfloat16)
        acc_s[...] = jnp.zeros_like(acc_s)
        for kind, ref in enumerate((q_ref, k_ref, v_ref)):
            for u, r in pieces:
                at = (u * RINGS + r) * part
                pltpu.make_async_copy(o_s.at[kind, :, pl.ds(at, part), :], ref.at[:, pl.ds(token(p, u, r), part), :], out_sem).start()

    events = (n - 1) * CUTS

    def event(e, _):
        slot = lax.rem(e, 2)

        @pl.when(e < events)
        def _():
            s, j, p, odd = task(e)
            arrive(s, j, s == n - 1)

            @pl.when(e == 0)
            def _():
                pltpu.make_async_copy(all_ref.at[:, pl.ds(0, rows), :], all_ref.at[:, pl.ds(0, rows), :], own_sem).wait()
                sent(0, 0)
                sent(0, 1)

            @pl.when(e == 1)
            def _():
                sent(0, 2)
                sent(0, 3)

            for u, r in pieces:
                pltpu.make_async_copy(all_ref.at[j, pl.ds(token(p, u, r), part), :], a_s.at[slot, pl.ds((u * RINGS + r) * part, part), :],
                                      load_sem.at[slot]).start()

            @pl.when(odd & (j == 1))
            def _():
                for u, r in pieces:
                    pltpu.make_async_copy(cs_ref.at[pl.ds(token(p, u, r), part), :], cs_s.at[pl.ds((u * RINGS + r) * part, part), :], cs_sem).start()

        @pl.when(e > 0)
        def _():
            s, j, p, odd = task(e - 1)
            final = s == n - 1

            @pl.when(s == 1)
            def _():
                pltpu.make_async_copy(w_s.at[columns(j), :], w_s.at[columns(j), :], w_sem.at[j]).wait()

            pltpu.make_async_copy(a_s.at[1 - slot], a_s.at[1 - slot], load_sem.at[1 - slot]).wait()

            def section(i, _):
                at = pl.ds(pl.multiple_of(i * one, one), one)
                acc_s[:, at] += _dot(a_s[1 - slot], w_s[columns(j), at], 1, 0)

            lax.fori_loop(jnp.where(odd, 0, 1), jnp.where(odd & jnp.logical_not(final), 1, 3), section, None)

            @pl.when((j == CUTS - 1) & (jnp.logical_not(odd) | final))
            def _():
                finish(p)

    lax.fori_loop(0, events + 1, event, None)
    written()

    def drain(s, _):
        for j in range(CUTS):
            sent(s, j)

    lax.fori_loop(1, n - 1, drain, None)


def gather_project(x, gain, cs, wq, wk, wv, n):
    rows, depth = x.shape
    one = wq.shape[1]
    heads = one // HEAD
    hbm = pl.BlockSpec(memory_space=pltpu.HBM)
    vmem = pl.BlockSpec(memory_space=pltpu.VMEM)
    dma = pltpu.SemaphoreType.DMA
    head = jax.ShapeDtypeStruct((heads, n * rows, HEAD), jnp.bfloat16)
    return pl.pallas_call(
        functools.partial(_gather_kernel, n),
        out_shape=[jax.ShapeDtypeStruct((CUTS, n * rows, depth // CUTS), jnp.bfloat16), head, head, head],
        in_specs=[hbm, vmem, hbm, hbm, hbm, hbm],
        out_specs=[hbm] * 4,
        scratch_shapes=[
            pltpu.VMEM((depth, 3 * one), jnp.bfloat16),
            pltpu.VMEM((2 * rows, 3 * one), jnp.float32),
            pltpu.VMEM((2, 2 * rows, depth // CUTS), jnp.bfloat16),
            pltpu.VMEM((3, heads, 2 * rows, HEAD), jnp.bfloat16),
            pltpu.VMEM((2 * rows, HEAD), jnp.float32),
            dma((RINGS,)), dma((CUTS,)), dma(()), dma((n, CUTS)), dma((n, CUTS)), dma((2,)), dma(()), dma(()),
        ],
        compiler_params=pltpu.CompilerParams(collective_id=0, has_side_effects=True, vmem_limit_bytes=FULL),
        cost_estimate=pl.CostEstimate(flops=6 * n * rows * depth * one, bytes_accessed=10 * n * rows * depth, transcendentals=0),
        name="gather_project",
    )(x, gain.reshape(1, depth), cs, wq, wk, wv)


SLOTS = 4


KEYS = 512


def _scatter_kernel(n, q_ref, k_ref, v_ref, wo_ref, x_ref, y_ref, wo_s, q_s, k_s, v_s, in_s, out_s, lhs_s, term_s, x_s, some_s, top_s, total_s, mix_s, place_s,
                    in_sem, wo_sem, x_sem, send_sem, recv_sem, y_sem, free_sem):
    side = math.isqrt(n)
    me = lax.axis_index("tp")
    rows, depth = x_ref.shape
    part = rows // RINGS
    width = depth // CUTS
    heads = q_ref.shape[0]
    e = HEAD**-0.5 * LOG2E
    ready = _greet(me, side)

    def columns(j):
        return pl.ds(pl.multiple_of(j * width, width), width)

    given = [pltpu.make_async_copy(a, b, in_sem.at[i]) for i, (a, b) in enumerate(((q_ref, q_s), (k_ref, k_s), (v_ref, v_s)))]
    for c in given:
        c.start()
    for j in range(CUTS):
        pltpu.make_async_copy(wo_ref.at[:, columns(j)], wo_s.at[j], wo_sem.at[j]).start()
    for j in range(CUTS):
        pltpu.make_async_copy(x_ref.at[:, columns(j)], x_s.at[j], x_sem).start()
    for c in given:
        c.wait()
    ready()

    def whole(s, slot, j):
        pltpu.make_async_copy(out_s.at[0, 0], out_s.at[0, 0], s.at[slot, j]).wait()

    def attended(s):
        starts = [pl.multiple_of(_ring(me, r, -(s + 1), side) * rows + r * part, part) for r in range(RINGS)]
        row = lax.broadcasted_iota(jnp.int32, (part, HEAD), 0)
        for r, at in enumerate(starts):
            place_s[r * part : (r + 1) * part, :] = row + at
            for h in range(heads):
                some_s[h, r * part : (r + 1) * part, :] = q_s[h, pl.ds(at, part), :]
        top_s[...] = jnp.full_like(top_s, NEG)
        total_s[...] = jnp.zeros_like(total_s)
        mix_s[...] = jnp.zeros_like(mix_s)

        def wide(t):
            return jnp.concatenate([t] * (KEYS // HEAD), axis=1)

        def block(c, _):
            here = pl.ds(pl.multiple_of(c * KEYS, KEYS), KEYS)
            hidden = lax.broadcasted_iota(jnp.int32, (rows, KEYS), 1) + c * KEYS > wide(place_s[...])
            scores = [_dot(some_s[h], k_s[h, here, :], 1, 1) for h in range(heads)]
            weights = []
            for h, s in enumerate(scores):
                s = jnp.where(hidden, HIDDEN, s)
                old = top_s[h]
                top = jnp.maximum(old, jnp.max(s, axis=1, keepdims=True))
                top_s[h] = top
                keep = jnp.exp2((old - top) * e)
                p = jnp.exp2((s - wide(top)) * e)
                total_s[h] = total_s[h] * keep + jnp.sum(p, axis=1, keepdims=True)
                weights.append((p.astype(jnp.bfloat16), keep))
            for h, (p, keep) in enumerate(weights):
                mix_s[h] = mix_s[h] * keep + _dot(p, v_s[h, here, :], 1, 0)

        last = functools.reduce(jnp.maximum, starts) + part
        lax.fori_loop(0, lax.div(last + KEYS - 1, KEYS), block, None)
        for h in range(heads):
            lhs_s[:, h * HEAD : (h + 1) * HEAD] = (mix_s[h] / total_s[h]).astype(jnp.bfloat16)

    def step(s, _):
        attended(s)
        slot, to, here = lax.rem(s, 2), lax.rem(s + 1, SLOTS), lax.rem(s, SLOTS)

        @pl.when((s >= SLOTS) & (s < n - 1))
        def _():
            for r in range(RINGS):
                pl.semaphore_wait(free_sem.at[r], 1)

        def cut(j, _):
            @pl.when(s == 0)
            def _():
                pltpu.make_async_copy(wo_s.at[j], wo_s.at[j], wo_sem.at[j]).wait()

            term_s[...] = _dot(lhs_s[...], wo_s[j], 1, 0)

            @pl.when(s >= 2)
            def _():
                whole(send_sem, slot, j)

            @pl.when(s == 0)
            def _():
                out_s[slot, j] = term_s[...].astype(jnp.bfloat16)

            @pl.when(s > 0)
            def _():
                whole(recv_sem, here, j)

            @pl.when((s > 0) & (s < n - 1))
            def _():
                out_s[slot, j] = (term_s[...] + in_s[here, j].astype(jnp.float32)).astype(jnp.bfloat16)

            @pl.when(s < n - 1)
            def _():
                for r in range(RINGS):
                    mine = pl.ds(r * part, part)
                    pltpu.make_async_remote_copy(src_ref=out_s.at[slot, j, mine, :], dst_ref=in_s.at[to, j, mine, :], send_sem=send_sem.at[slot, j],
                                                 recv_sem=recv_sem.at[to, j], device_id={"tp": _ring(me, r, 1, side)}, device_id_type=MESH_ID).start()

            @pl.when(s == n - 1)
            def _():
                @pl.when(j == 0)
                def _():
                    pltpu.make_async_copy(x_s, x_s, x_sem).wait()

                sums = term_s[...] + in_s[here, j].astype(jnp.float32)
                out_s[slot, j] = (x_s[j].astype(jnp.float32) + sums).astype(jnp.bfloat16)
                pltpu.make_async_copy(out_s.at[slot, j], y_ref.at[:, columns(j)], y_sem).start()

        lax.fori_loop(0, CUTS, cut, None)

        @pl.when((s > 0) & (s < n - SLOTS))
        def _():
            for r in range(RINGS):
                pl.semaphore_signal(free_sem.at[r], inc=1, device_id={"tp": _ring(me, r, -1, side)}, device_id_type=MESH_ID)

    lax.fori_loop(0, n, step, None)
    for j in range(CUTS):
        whole(send_sem, (n - 2) % 2, j)
    pltpu.make_async_copy(out_s.at[0], out_s.at[0], y_sem).wait()


def attend_project_scatter(q, k, v, wo, x, n):
    rows, depth = x.shape
    heads = q.shape[0]
    state = pltpu.VMEM((heads, rows, HEAD), jnp.float32)
    hbm = pl.BlockSpec(memory_space=pltpu.HBM)
    dma = pltpu.SemaphoreType.DMA
    width = depth // CUTS
    return pl.pallas_call(
        functools.partial(_scatter_kernel, n),
        out_shape=jax.ShapeDtypeStruct((rows, depth), jnp.bfloat16),
        in_specs=[hbm] * 5,
        out_specs=hbm,
        scratch_shapes=[
            pltpu.VMEM((CUTS, heads * HEAD, width), jnp.bfloat16),
            *[pltpu.VMEM(q.shape, jnp.bfloat16)] * 3,
            pltpu.VMEM((SLOTS, CUTS, rows, width), jnp.bfloat16),
            pltpu.VMEM((2, CUTS, rows, width), jnp.bfloat16),
            pltpu.VMEM((rows, heads * HEAD), jnp.bfloat16),
            pltpu.VMEM((rows, width), jnp.float32),
            pltpu.VMEM((CUTS, rows, width), jnp.bfloat16),
            pltpu.VMEM((heads, rows, HEAD), jnp.bfloat16), state, state, state,
            pltpu.VMEM((rows, HEAD), jnp.int32),
            dma((3,)), dma((CUTS,)), dma(()), dma((2, CUTS)), dma((SLOTS, CUTS)), dma(()), pltpu.SemaphoreType.REGULAR((RINGS,)),
        ],
        compiler_params=pltpu.CompilerParams(collective_id=1, has_side_effects=True, vmem_limit_bytes=FULL),
        cost_estimate=pl.CostEstimate(flops=2 * n * rows * depth * heads * HEAD, bytes_accessed=4 * n * rows * depth, transcendentals=0),
        name="attend_project_scatter",
    )(q, k, v, wo, x)


def _turns(rows):
    half = HEAD // 2
    angle = np.arange(rows, dtype=np.float32)[:, None] * np.float32(THETA) ** (-np.arange(half, dtype=np.float32) / np.float32(half))
    return np.concatenate([np.cos(angle), np.sin(angle)], -1).astype(np.float32)


def solution(mesh):
    n = mesh.shape["tp"]

    def step(x, gain, wq, wk, wv, wo):
        _, q, k, v = gather_project(x, gain, jnp.asarray(_turns(n * x.shape[0])), wq, wk, wv, n)
        return attend_project_scatter(q, k, v, wo, x, n)

    tokens, columns = P(("dp", "tp"), None), P(None, "tp")
    return jax.shard_map(
        step,
        mesh=mesh,
        in_specs=(tokens, P(None), columns, columns, columns, P("tp", None)),
        out_specs=tokens,
        check_vma=False,
    )
```

```python
import functools

import jax
import jax.numpy as jnp
from jax import lax
from jax.experimental import pallas as pl
from jax.experimental.pallas import tpu as pltpu

NEG = -1e30
HIDDEN = 2 * NEG
LOG2E = 1.4426950408889634


def _dot(a, b, ca, cb):
    return lax.dot_general(a, b, (((ca,), (cb,)), ((), ())), preferred_element_type=jnp.float32)


import math

import numpy as np
from jax.sharding import PartitionSpec as P

HEAD = 128
THETA = 10000
RINGS = 4
CUTS = 8
HELD = CUTS // 2
FULL = 67043328
MESH_ID = pl.DeviceIdType.MESH


def _place(me, cycle, side):
    x, y = lax.div(me, side), lax.rem(me, side)
    return (y * side if cycle else x * side) + lax.rem(x + y, side)


def _device(place, cycle, side):
    place = lax.rem(place, side * side)
    i, k = lax.div(place, side), lax.rem(place, side)
    j = lax.rem(k - i + side, side)
    return j * side + i if cycle else i * side + j


def _ring(me, r, hops, side):
    n = side * side
    cycle, back = divmod(r, 2)
    return _device(_place(me, cycle, side) + (2 * n - hops if back else 2 * n + hops), cycle, side)


def _greet(ahead):
    barrier = pltpu.get_barrier_semaphore()
    for d in ahead:
        pl.semaphore_signal(barrier, inc=1, device_id={"tp": d}, device_id_type=MESH_ID)
    return lambda: pl.semaphore_wait(barrier, RINGS)


def _gather_kernel(n, x_ref, gain_ref, cs_ref, wq_ref, wk_ref, wv_ref, all_ref, q_ref, k_ref, v_ref,
                   w_s, acc_s, a_s, o_s, cs_s, gain_s, x_sem, w_sem, own_sem, send_sem, recv_sem, load_sem, cs_sem, out_sem):
    side = math.isqrt(n)
    me = lax.axis_index("tp")
    rows, depth = x_ref.shape
    part = rows // RINGS
    width = depth // CUTS
    one = wq_ref.shape[1]
    heads = one // HEAD
    ahead = [_ring(me, r, 1, side) for r in range(RINGS)]
    ready = _greet(ahead)

    def columns(j):
        return pl.ds(pl.multiple_of(j * width, width), width)

    def home(j):
        return a_s.at[j // 2, pl.ds((j % 2) * rows, rows), :]

    for r in range(RINGS):
        for j in range(CUTS):
            pltpu.make_async_copy(x_ref.at[pl.ds(r * part, part), columns(j)], home(j).at[pl.ds(r * part, part), :], x_sem.at[r]).start()

    def token(s, r):
        return pl.multiple_of(_ring(me, r, -s, side) * rows + r * part, part)

    def remote(src, r, s, j, first):
        at = pl.ds(first, part)
        src = all_ref.at[j, at, :] if src is None else src
        return pltpu.make_async_remote_copy(src_ref=src, dst_ref=all_ref.at[j, at, :], send_sem=send_sem.at[s, j], recv_sem=recv_sem.at[s + 1, j],
                                            device_id={"tp": ahead[r]}, device_id_type=MESH_ID)

    gain_s[...] = gain_ref[...].astype(jnp.float32)
    for r in range(RINGS):
        pltpu.make_async_copy(a_s.at[0, pl.ds(0, CUTS * part), :], a_s.at[0, pl.ds(0, CUTS * part), :], x_sem.at[r]).wait()
        for g in range(0, part, 16):
            at = [(j // 2, (j % 2) * rows + r * part + g) for j in range(CUTS)]
            total = jnp.zeros((16, HEAD), jnp.float32)
            for c, t in at:
                for i in range(0, width, HEAD):
                    wide = a_s[c, t : t + 16, i : i + HEAD].astype(jnp.float32)
                    total += wide * wide
            scale = lax.rsqrt(jnp.sum(total, -1, keepdims=True) / depth + 1e-6)
            for j, (c, t) in enumerate(at):
                for i in range(0, width, HEAD):
                    wide = a_s[c, t : t + 16, i : i + HEAD].astype(jnp.float32)
                    at_gain = (j * width + i) // HEAD
                    a_s[c, t : t + 16, i : i + HEAD] = (wide * scale * gain_s[at_gain : at_gain + 1, :]).astype(jnp.bfloat16)
        if r == 0:
            ready()
        for j in range(CUTS):
            remote(home(j).at[pl.ds(r * part, part), :], r, 0, j, token(0, r)).start()
    own = [pltpu.make_async_copy(home(j), all_ref.at[j, pl.ds(pl.multiple_of(me * rows, rows), rows), :], own_sem) for j in range(CUTS)]
    for c in own:
        c.start()

    def weights(i, j):
        return pltpu.make_async_copy((wq_ref, wk_ref, wv_ref)[i].at[columns(j), :], w_s.at[columns(j), pl.ds(i * one, one)], w_sem.at[i, j])

    for j in range(CUTS):
        weights(0, j).start()
    acc_s[...] = jnp.zeros_like(acc_s)

    def sent(s, j):
        pltpu.make_async_copy(all_ref.at[0, pl.ds(0, rows), :], all_ref.at[0, pl.ds(0, rows), :], send_sem.at[s, j]).wait()

    pieces = [(u, r) for u in range(2) for r in range(RINGS)]

    def written():
        pltpu.make_async_copy(o_s, o_s, out_sem).wait()

    def finish(p):
        pl.when(p > 0)(written)
        pltpu.make_async_copy(cs_s, cs_s, cs_sem).wait()
        step = 64
        for t in range(0, 2 * rows, step):
            cs = cs_s[t : t + step, :]
            sc = pltpu.roll(cs, HEAD // 2, 1)
            low = lax.broadcasted_iota(jnp.int32, cs.shape, 1) < HEAD // 2
            cos, sin = jnp.where(low, cs, sc), jnp.where(low, -sc, cs)
            for h in range(3 * heads):
                got = acc_s[t : t + step, h * HEAD : (h + 1) * HEAD]
                if h < 2 * heads:
                    got = got.astype(jnp.bfloat16).astype(jnp.float32)
                    got = got * cos + pltpu.roll(got, HEAD // 2, 1) * sin
                o_s[h // heads, h % heads, t : t + step, :] = got.astype(jnp.bfloat16)
        acc_s[...] = jnp.zeros_like(acc_s)
        firsts = [token(2 * p + u, r) for u, r in pieces]
        for kind, ref in enumerate((q_ref, k_ref, v_ref)):
            for u, r in pieces:
                at = (u * RINGS + r) * part
                pltpu.make_async_copy(o_s.at[kind, :, pl.ds(at, part), :], ref.at[:, pl.ds(firsts[u * RINGS + r], part), :], out_sem).start()

    def step(s, _):
        p, odd = lax.div(s - 1, 2), lax.rem(s, 2) == 1
        here = [token(s, r) for r in range(RINGS)]
        firsts = [token(2 * p + u, r) for u, r in pieces]

        def piece(j, _):
            e = (s - 1) * CUTS + j
            slot, before = lax.rem(e, HELD), lax.rem(e + HELD - 1, HELD)

            @pl.when(s < n)
            def _():
                pltpu.make_async_copy(all_ref.at[0, pl.ds(0, rows), :], all_ref.at[0, pl.ds(0, rows), :], recv_sem.at[s, j]).wait()

                @pl.when(s < n - 1)
                def _():
                    for r in range(RINGS):
                        remote(None, r, s, j, here[r]).start()

                @pl.when(e == 0)
                def _():
                    pltpu.make_async_copy(all_ref.at[:, pl.ds(0, rows), :], all_ref.at[:, pl.ds(0, rows), :], own_sem).wait()

                @pl.when(e < HELD)
                def _():
                    sent(0, 2 * e)
                    sent(0, 2 * e + 1)

                @pl.when(e < CUTS)
                def _():
                    weights(1, e).start()
                    weights(2, e).start()

                for i in range(2 * RINGS):
                    pltpu.make_async_copy(all_ref.at[j, pl.ds(firsts[i], part), :], a_s.at[slot, pl.ds(i * part, part), :], load_sem.at[slot]).start()

                @pl.when(odd & (j == 1))
                def _():
                    for i in range(2 * RINGS):
                        pltpu.make_async_copy(cs_ref.at[pl.ds(firsts[i], part), :], cs_s.at[pl.ds(i * part, part), :], cs_sem).start()

            @pl.when(e > 0)
            def _():
                s = lax.div(e - 1, CUTS) + 1
                j, p, odd = lax.rem(e - 1, CUTS), lax.div(s - 1, 2), lax.rem(s, 2) == 1
                final = s == n - 1

                @pl.when(s == 1)
                def _():
                    weights(0, j).wait()

                @pl.when(s == 2)
                def _():
                    weights(1, j).wait()
                    weights(2, j).wait()

                pltpu.make_async_copy(a_s.at[before], a_s.at[before], load_sem.at[before]).wait()

                def section(i, _):
                    at = pl.ds(pl.multiple_of(i * one, one), one)
                    acc_s[:, at] += _dot(a_s[before], w_s[columns(j), at], 1, 0)

                lax.fori_loop(jnp.where(odd, 0, 1), jnp.where(odd & jnp.logical_not(final), 1, 3), section, None)

                @pl.when((j == CUTS - 1) & (jnp.logical_not(odd) | final))
                def _():
                    finish(p)

        lax.fori_loop(0, jnp.where(s < n, CUTS, 1), piece, None)

    lax.fori_loop(1, n + 1, step, None)
    written()

    def drain(s, _):
        for j in range(CUTS):
            sent(s, j)

    lax.fori_loop(1, n - 1, drain, None)


def gather_project(x, gain, cs, wq, wk, wv, n):
    rows, depth = x.shape
    one = wq.shape[1]
    heads = one // HEAD
    hbm = pl.BlockSpec(memory_space=pltpu.HBM)
    vmem = pl.BlockSpec(memory_space=pltpu.VMEM)
    dma = pltpu.SemaphoreType.DMA
    head = jax.ShapeDtypeStruct((heads, n * rows, HEAD), jnp.bfloat16)
    return pl.pallas_call(
        functools.partial(_gather_kernel, n),
        out_shape=[jax.ShapeDtypeStruct((CUTS, n * rows, depth // CUTS), jnp.bfloat16), head, head, head],
        in_specs=[hbm, vmem, hbm, hbm, hbm, hbm],
        out_specs=[hbm] * 4,
        scratch_shapes=[
            pltpu.VMEM((depth, 3 * one), jnp.bfloat16),
            pltpu.VMEM((2 * rows, 3 * one), jnp.float32),
            pltpu.VMEM((HELD, 2 * rows, depth // CUTS), jnp.bfloat16),
            pltpu.VMEM((3, heads, 2 * rows, HEAD), jnp.bfloat16),
            pltpu.VMEM((2 * rows, HEAD), jnp.float32),
            pltpu.VMEM((depth // HEAD, HEAD), jnp.float32),
            dma((RINGS,)), dma((3, CUTS)), dma(()), dma((n, CUTS)), dma((n, CUTS)), dma((HELD,)), dma(()), dma(()),
        ],
        compiler_params=pltpu.CompilerParams(collective_id=0, has_side_effects=True, vmem_limit_bytes=FULL),
        cost_estimate=pl.CostEstimate(flops=6 * n * rows * depth * one, bytes_accessed=10 * n * rows * depth, transcendentals=0),
        name="gather_project",
    )(x, gain.reshape(-1, HEAD), cs, wq, wk, wv)


SLOTS = 4


KEYS = 512


def _scatter_kernel(n, q_ref, k_ref, v_ref, wo_ref, x_ref, y_ref, wo_s, q_s, k_s, v_s, in_s, out_s, lhs_s, term_s, x_s, some_s, top_s, total_s, mix_s, place_s,
                    q_sem, in_sem, wo_sem, x_sem, send_sem, recv_sem, free_sem):
    side = math.isqrt(n)
    me = lax.axis_index("tp")
    rows, depth = x_ref.shape
    part = rows // RINGS
    width = depth // CUTS
    heads = q_ref.shape[0]
    e = HEAD**-0.5 * LOG2E
    ahead = [_ring(me, r, 1, side) for r in range(RINGS)]
    ready = _greet(ahead)

    def columns(j):
        return pl.ds(pl.multiple_of(j * width, width), width)

    blocks = q_ref.shape[1] // KEYS

    def given(c):
        here = pl.ds(pl.multiple_of(c * KEYS, KEYS), KEYS)
        return [pltpu.make_async_copy(a.at[:, here, :], b.at[:, here, :], in_sem.at[i, c]) for i, (a, b) in enumerate(((k_ref, k_s), (v_ref, v_s)))]

    asked = pltpu.make_async_copy(q_ref, q_s, q_sem)
    asked.start()
    for c in range(blocks):
        for copy in given(c):
            copy.start()
    asked.wait()
    ready()

    def fetch():
        for j in range(CUTS):
            pltpu.make_async_copy(wo_ref.at[:, columns(j)], wo_s.at[j], wo_sem.at[j]).start()
        for j in range(CUTS):
            pltpu.make_async_copy(x_ref.at[:, columns(j)], x_s.at[j], x_sem).start()

    def whole(s, slot, j):
        pltpu.make_async_copy(out_s.at[0, 0], out_s.at[0, 0], s.at[slot, j]).wait()

    def attended(s):
        starts = [pl.multiple_of(_ring(me, r, -(s + 1), side) * rows + r * part, part) for r in range(RINGS)]
        row = lax.broadcasted_iota(jnp.int32, (part, HEAD), 0)
        for r, at in enumerate(starts):
            place_s[r * part : (r + 1) * part, :] = row + at
            for h in range(heads):
                some_s[h, r * part : (r + 1) * part, :] = q_s[h, pl.ds(at, part), :]
        top_s[...] = jnp.full_like(top_s, NEG)
        total_s[...] = jnp.zeros_like(total_s)
        mix_s[...] = jnp.zeros_like(mix_s)

        def wide(t):
            return jnp.concatenate([t] * (KEYS // HEAD), axis=1)

        def block(c, _):
            pl.when(s == 0)(lambda: [copy.wait() for copy in given(c)] and None)
            here = pl.ds(pl.multiple_of(c * KEYS, KEYS), KEYS)
            hidden = lax.broadcasted_iota(jnp.int32, (rows, KEYS), 1) + c * KEYS > wide(place_s[...])
            scores = [_dot(some_s[h], k_s[h, here, :], 1, 1) for h in range(heads)]
            weights = []
            for h, t in enumerate(scores):
                t = jnp.where(hidden, HIDDEN, t)
                old = top_s[h]
                top = jnp.maximum(old, jnp.max(t, axis=1, keepdims=True))
                top_s[h] = top
                keep = jnp.exp2((old - top) * e)
                p = jnp.exp2((t - wide(top)) * e)
                total_s[h] = total_s[h] * keep + jnp.sum(p, axis=1, keepdims=True)
                weights.append((p.astype(jnp.bfloat16), keep))
            for h, (p, keep) in enumerate(weights):
                mix_s[h] = mix_s[h] * keep + _dot(p, v_s[h, here, :], 1, 0)
            pl.when((s == 0) & (c == 0))(fetch)

        last = lax.div(functools.reduce(jnp.maximum, starts) + part + KEYS - 1, KEYS)
        lax.fori_loop(0, last, block, None)

        def rest(c, _):
            for copy in given(c):
                copy.wait()

        pl.when(s == 0)(lambda: lax.fori_loop(last, blocks, rest, None))
        for h in range(heads):
            lhs_s[:, h * HEAD : (h + 1) * HEAD] = (mix_s[h] / total_s[h]).astype(jnp.bfloat16)

    def step(s, _):
        attended(s)
        slot, to, here = lax.rem(s, 2), lax.rem(s + 1, SLOTS), lax.rem(s, SLOTS)

        @pl.when((s >= SLOTS) & (s < n - 1))
        def _():
            for r in range(RINGS):
                pl.semaphore_wait(free_sem.at[r], 1)

        def cut(j, _):
            @pl.when(s == 0)
            def _():
                pltpu.make_async_copy(wo_s.at[j], wo_s.at[j], wo_sem.at[j]).wait()

            term_s[...] = _dot(lhs_s[...], wo_s[j], 1, 0)

            @pl.when(s >= 2)
            def _():
                whole(send_sem, slot, j)

            @pl.when(s == 0)
            def _():
                out_s[slot, j] = term_s[...].astype(jnp.bfloat16)

            @pl.when(s > 0)
            def _():
                whole(recv_sem, here, j)

            @pl.when((s > 0) & (s < n - 1))
            def _():
                out_s[slot, j] = (term_s[...] + in_s[here, j].astype(jnp.float32)).astype(jnp.bfloat16)

            @pl.when(s < n - 1)
            def _():
                for r in range(RINGS):
                    mine = pl.ds(r * part, part)
                    pltpu.make_async_remote_copy(src_ref=out_s.at[slot, j, mine, :], dst_ref=in_s.at[to, j, mine, :], send_sem=send_sem.at[slot, j],
                                                 recv_sem=recv_sem.at[to, j], device_id={"tp": ahead[r]}, device_id_type=MESH_ID).start()

            @pl.when(s == n - 1)
            def _():
                @pl.when(j == 0)
                def _():
                    pltpu.make_async_copy(x_s, x_s, x_sem).wait()

                sums = term_s[...] + in_s[here, j].astype(jnp.float32)
                y_ref[:, columns(j)] = (x_s[j].astype(jnp.float32) + sums).astype(jnp.bfloat16)

        lax.fori_loop(0, CUTS, cut, None)

        @pl.when((s > 0) & (s < n - SLOTS))
        def _():
            for r in range(RINGS):
                pl.semaphore_signal(free_sem.at[r], inc=1, device_id={"tp": ahead[r ^ 1]}, device_id_type=MESH_ID)

    lax.fori_loop(0, n, step, None)
    for j in range(CUTS):
        whole(send_sem, (n - 2) % 2, j)


def attend_project_scatter(q, k, v, wo, x, n):
    rows, depth = x.shape
    heads = q.shape[0]
    state = pltpu.VMEM((heads, rows, HEAD), jnp.float32)
    hbm = pl.BlockSpec(memory_space=pltpu.HBM)
    dma = pltpu.SemaphoreType.DMA
    width = depth // CUTS
    return pl.pallas_call(
        functools.partial(_scatter_kernel, n),
        out_shape=pltpu.VMEM((rows, depth), jnp.bfloat16),
        in_specs=[hbm] * 5,
        out_specs=pl.BlockSpec(memory_space=pltpu.VMEM),
        scratch_shapes=[
            pltpu.VMEM((CUTS, heads * HEAD, width), jnp.bfloat16),
            *[pltpu.VMEM(q.shape, jnp.bfloat16)] * 3,
            pltpu.VMEM((SLOTS, CUTS, rows, width), jnp.bfloat16),
            pltpu.VMEM((2, CUTS, rows, width), jnp.bfloat16),
            pltpu.VMEM((rows, heads * HEAD), jnp.bfloat16),
            pltpu.VMEM((rows, width), jnp.float32),
            pltpu.VMEM((CUTS, rows, width), jnp.bfloat16),
            pltpu.VMEM((heads, rows, HEAD), jnp.bfloat16), state, state, state,
            pltpu.VMEM((rows, HEAD), jnp.int32),
            dma(()), dma((2, n * rows // KEYS)), dma((CUTS,)), dma(()), dma((2, CUTS)), dma((SLOTS, CUTS)), pltpu.SemaphoreType.REGULAR((RINGS,)),
        ],
        compiler_params=pltpu.CompilerParams(collective_id=1, has_side_effects=True, vmem_limit_bytes=59 * 2**20),
        cost_estimate=pl.CostEstimate(flops=2 * n * rows * depth * heads * HEAD, bytes_accessed=4 * n * rows * depth, transcendentals=0),
        name="attend_project_scatter",
    )(q, k, v, wo, x)


def _turns(rows):
    half = HEAD // 2
    angle = np.arange(rows, dtype=np.float32)[:, None] * np.float32(THETA) ** (-np.arange(half, dtype=np.float32) / np.float32(half))
    return np.concatenate([np.cos(angle), np.sin(angle)], -1).astype(np.float32)


def solution(mesh):
    n = mesh.shape["tp"]

    def step(x, gain, wq, wk, wv, wo):
        _, q, k, v = gather_project(x, gain, jnp.asarray(_turns(n * x.shape[0])), wq, wk, wv, n)
        return attend_project_scatter(q, k, v, wo, x, n)

    tokens, columns = P(("dp", "tp"), None), P(None, "tp")
    return jax.shard_map(
        step,
        mesh=mesh,
        in_specs=(tokens, P(None), columns, columns, columns, P("tp", None)),
        out_specs=tokens,
        check_vma=False,
    )
```

```python
import functools

import jax
import jax.numpy as jnp
from jax import lax
from jax.experimental import pallas as pl
from jax.experimental.pallas import tpu as pltpu

NEG = -1e30
HIDDEN = 2 * NEG
LOG2E = 1.4426950408889634


def _dot(a, b, ca, cb):
    return lax.dot_general(a, b, (((ca,), (cb,)), ((), ())), preferred_element_type=jnp.float32)


import math

import numpy as np
from jax.sharding import PartitionSpec as P

HEAD = 128
THETA = 10000
RINGS = 4
CUTS = 8
HELD = CUTS // 2
FULL = 67043328
MESH_ID = pl.DeviceIdType.MESH


def _place(me, cycle, side):
    x, y = lax.div(me, side), lax.rem(me, side)
    return (y * side if cycle else x * side) + lax.rem(x + y, side)


def _device(place, cycle, side):
    place = lax.rem(place, side * side)
    i, k = lax.div(place, side), lax.rem(place, side)
    j = lax.rem(k - i + side, side)
    return j * side + i if cycle else i * side + j


def _ring(me, r, hops, side):
    n = side * side
    cycle, back = divmod(r, 2)
    return _device(_place(me, cycle, side) + (2 * n - hops if back else 2 * n + hops), cycle, side)


def _greet(ahead):
    barrier = pltpu.get_barrier_semaphore()
    for d in ahead:
        pl.semaphore_signal(barrier, inc=1, device_id={"tp": d}, device_id_type=MESH_ID)
    return lambda: pl.semaphore_wait(barrier, RINGS)


def _gather_kernel(n, x_ref, gain_ref, cs_ref, wq_ref, wk_ref, wv_ref, all_ref, q_ref, k_ref, v_ref,
                   w_s, acc_s, a_s, o_s, cs_s, gain_s, x_sem, w_sem, own_sem, send_sem, recv_sem, load_sem, cs_sem, out_sem):
    side = math.isqrt(n)
    me = lax.axis_index("tp")
    rows, depth = x_ref.shape
    part = rows // RINGS
    width = depth // CUTS
    one = wq_ref.shape[1]
    heads = one // HEAD
    ahead = [_ring(me, r, 1, side) for r in range(RINGS)]
    ready = _greet(ahead)

    def columns(j):
        return pl.ds(pl.multiple_of(j * width, width), width)

    def home(j):
        return a_s.at[j // 2, pl.ds((j % 2) * rows, rows), :]

    for r in range(RINGS):
        for j in range(CUTS):
            pltpu.make_async_copy(x_ref.at[pl.ds(r * part, part), columns(j)], home(j).at[pl.ds(r * part, part), :], x_sem.at[r]).start()

    def token(s, r):
        return pl.multiple_of(_ring(me, r, -s, side) * rows + r * part, part)

    def remote(src, r, s, j, first):
        at = pl.ds(first, part)
        src = all_ref.at[j, at, :] if src is None else src
        return pltpu.make_async_remote_copy(src_ref=src, dst_ref=all_ref.at[j, at, :], send_sem=send_sem.at[s, j], recv_sem=recv_sem.at[s + 1, j],
                                            device_id={"tp": ahead[r]}, device_id_type=MESH_ID)

    gain_s[...] = gain_ref[...].astype(jnp.float32)
    for r in range(RINGS):
        pltpu.make_async_copy(a_s.at[0, pl.ds(0, CUTS * part), :], a_s.at[0, pl.ds(0, CUTS * part), :], x_sem.at[r]).wait()
        for g in range(0, part, 16):
            at = [(j // 2, (j % 2) * rows + r * part + g) for j in range(CUTS)]
            total = jnp.zeros((16, HEAD), jnp.float32)
            for c, t in at:
                for i in range(0, width, HEAD):
                    wide = a_s[c, t : t + 16, i : i + HEAD].astype(jnp.float32)
                    total += wide * wide
            scale = lax.rsqrt(jnp.sum(total, -1, keepdims=True) / depth + 1e-6)
            for j, (c, t) in enumerate(at):
                for i in range(0, width, HEAD):
                    wide = a_s[c, t : t + 16, i : i + HEAD].astype(jnp.float32)
                    at_gain = (j * width + i) // HEAD
                    a_s[c, t : t + 16, i : i + HEAD] = (wide * scale * gain_s[at_gain : at_gain + 1, :]).astype(jnp.bfloat16)
        if r == 0:
            ready()
        for j in range(CUTS):
            remote(home(j).at[pl.ds(r * part, part), :], r, 0, j, token(0, r)).start()
    own = [pltpu.make_async_copy(home(j), all_ref.at[j, pl.ds(pl.multiple_of(me * rows, rows), rows), :], own_sem) for j in range(CUTS)]
    for c in own:
        c.start()

    def weights(i, j):
        return pltpu.make_async_copy((wq_ref, wk_ref, wv_ref)[i].at[columns(j), :], w_s.at[columns(j), pl.ds(i * one, one)], w_sem.at[i, j])

    for j in range(CUTS):
        weights(0, j).start()
    acc_s[...] = jnp.zeros_like(acc_s)

    def sent(s, j):
        pltpu.make_async_copy(all_ref.at[0, pl.ds(0, rows), :], all_ref.at[0, pl.ds(0, rows), :], send_sem.at[s, j]).wait()

    pieces = [(u, r) for u in range(2) for r in range(RINGS)]

    def written():
        pltpu.make_async_copy(o_s, o_s, out_sem).wait()

    def finish(p):
        pl.when(p > 0)(written)
        pltpu.make_async_copy(cs_s, cs_s, cs_sem).wait()
        firsts = [token(2 * p + u, r) for u, r in pieces]
        step = 64
        for kind, ref in enumerate((q_ref, k_ref, v_ref)):
            for t in range(0, 2 * rows, step):
                cs = cs_s[t : t + step, :]
                sc = pltpu.roll(cs, HEAD // 2, 1)
                low = lax.broadcasted_iota(jnp.int32, cs.shape, 1) < HEAD // 2
                cos, sin = jnp.where(low, cs, sc), jnp.where(low, -sc, cs)
                for h in range(heads):
                    at = kind * one + h * HEAD
                    got = acc_s[t : t + step, at : at + HEAD]
                    if kind < 2:
                        got = got.astype(jnp.bfloat16).astype(jnp.float32)
                        got = got * cos + pltpu.roll(got, HEAD // 2, 1) * sin
                    o_s[kind, h, t : t + step, :] = got.astype(jnp.bfloat16)
            for i in range(2 * RINGS):
                pltpu.make_async_copy(o_s.at[kind, :, pl.ds(i * part, part), :], ref.at[:, pl.ds(firsts[i], part), :], out_sem).start()
        acc_s[...] = jnp.zeros_like(acc_s)

    def step(s, _):
        p, odd = lax.div(s - 1, 2), lax.rem(s, 2) == 1
        here = [token(s, r) for r in range(RINGS)]
        firsts = [token(2 * p + u, r) for u, r in pieces]

        def piece(j, _):
            e = (s - 1) * CUTS + j
            slot, before = lax.rem(e, HELD), lax.rem(e + HELD - 1, HELD)

            @pl.when(s < n)
            def _():
                pltpu.make_async_copy(all_ref.at[0, pl.ds(0, rows), :], all_ref.at[0, pl.ds(0, rows), :], recv_sem.at[s, j]).wait()

                @pl.when(s < n - 1)
                def _():
                    for r in range(RINGS):
                        remote(None, r, s, j, here[r]).start()

                @pl.when(e == 0)
                def _():
                    pltpu.make_async_copy(all_ref.at[:, pl.ds(0, rows), :], all_ref.at[:, pl.ds(0, rows), :], own_sem).wait()

                @pl.when(e < HELD)
                def _():
                    sent(0, 2 * e)
                    sent(0, 2 * e + 1)

                @pl.when(e < CUTS)
                def _():
                    weights(1, e).start()
                    weights(2, e).start()

                for i in range(2 * RINGS):
                    pltpu.make_async_copy(all_ref.at[j, pl.ds(firsts[i], part), :], a_s.at[slot, pl.ds(i * part, part), :], load_sem.at[slot]).start()

                @pl.when(odd & (j == 1))
                def _():
                    for i in range(2 * RINGS):
                        pltpu.make_async_copy(cs_ref.at[pl.ds(firsts[i], part), :], cs_s.at[pl.ds(i * part, part), :], cs_sem).start()

            @pl.when(e > 0)
            def _():
                s = lax.div(e - 1, CUTS) + 1
                j, p, odd = lax.rem(e - 1, CUTS), lax.div(s - 1, 2), lax.rem(s, 2) == 1
                final = s == n - 1

                @pl.when(s == 1)
                def _():
                    weights(0, j).wait()

                @pl.when(s == 2)
                def _():
                    weights(1, j).wait()
                    weights(2, j).wait()

                pltpu.make_async_copy(a_s.at[before], a_s.at[before], load_sem.at[before]).wait()

                def sections(first, last):
                    for i in range(first, last):
                        at = slice(i * one, (i + 1) * one)
                        acc_s[:, at] += _dot(a_s[before], w_s[columns(j), at], 1, 0)

                pl.when(odd & jnp.logical_not(final))(lambda: sections(0, 1))
                pl.when(jnp.logical_not(odd))(lambda: sections(1, 3))
                pl.when(final)(lambda: sections(0, 3))

                @pl.when((j == CUTS - 1) & (jnp.logical_not(odd) | final))
                def _():
                    finish(p)

        lax.fori_loop(0, jnp.where(s < n, CUTS, 1), piece, None)

    lax.fori_loop(1, n + 1, step, None)
    written()

    def drain(s, _):
        for j in range(CUTS):
            sent(s, j)

    lax.fori_loop(1, n - 1, drain, None)


def gather_project(x, gain, cs, wq, wk, wv, n):
    rows, depth = x.shape
    one = wq.shape[1]
    heads = one // HEAD
    hbm = pl.BlockSpec(memory_space=pltpu.HBM)
    vmem = pl.BlockSpec(memory_space=pltpu.VMEM)
    dma = pltpu.SemaphoreType.DMA
    head = jax.ShapeDtypeStruct((heads, n * rows, HEAD), jnp.bfloat16)
    return pl.pallas_call(
        functools.partial(_gather_kernel, n),
        out_shape=[jax.ShapeDtypeStruct((CUTS, n * rows, depth // CUTS), jnp.bfloat16), head, head, head],
        in_specs=[hbm, vmem, hbm, hbm, hbm, hbm],
        out_specs=[hbm] * 4,
        scratch_shapes=[
            pltpu.VMEM((depth, 3 * one), jnp.bfloat16),
            pltpu.VMEM((2 * rows, 3 * one), jnp.float32),
            pltpu.VMEM((HELD, 2 * rows, depth // CUTS), jnp.bfloat16),
            pltpu.VMEM((3, heads, 2 * rows, HEAD), jnp.bfloat16),
            pltpu.VMEM((2 * rows, HEAD), jnp.float32),
            pltpu.VMEM((depth // HEAD, HEAD), jnp.float32),
            dma((RINGS,)), dma((3, CUTS)), dma(()), dma((n, CUTS)), dma((n, CUTS)), dma((HELD,)), dma(()), dma(()),
        ],
        compiler_params=pltpu.CompilerParams(collective_id=0, has_side_effects=True, vmem_limit_bytes=FULL),
        cost_estimate=pl.CostEstimate(flops=6 * n * rows * depth * one, bytes_accessed=10 * n * rows * depth, transcendentals=0),
        name="gather_project",
    )(x, gain.reshape(-1, HEAD), cs, wq, wk, wv)


SLOTS = 4


KEYS = 512


def _scatter_kernel(n, q_ref, k_ref, v_ref, wo_ref, x_ref, y_ref, wo_s, q_s, k_s, v_s, in_s, out_s, lhs_s, term_s, x_s, some_s, top_s, total_s, mix_s, place_s,
                    q_sem, in_sem, wo_sem, x_sem, send_sem, recv_sem, free_sem):
    side = math.isqrt(n)
    me = lax.axis_index("tp")
    rows, depth = x_ref.shape
    part = rows // RINGS
    width = depth // CUTS
    heads = q_ref.shape[0]
    e = HEAD**-0.5 * LOG2E
    ahead = [_ring(me, r, 1, side) for r in range(RINGS)]
    ready = _greet(ahead)

    def columns(j):
        return pl.ds(pl.multiple_of(j * width, width), width)

    blocks = q_ref.shape[1] // KEYS

    def given(c):
        here = pl.ds(pl.multiple_of(c * KEYS, KEYS), KEYS)
        return [pltpu.make_async_copy(a.at[:, here, :], b.at[:, here, :], in_sem.at[i, c]) for i, (a, b) in enumerate(((k_ref, k_s), (v_ref, v_s)))]

    asked = pltpu.make_async_copy(q_ref, q_s, q_sem)
    asked.start()
    for c in range(blocks):
        for copy in given(c):
            copy.start()
    asked.wait()
    ready()

    def fetch():
        for j in range(CUTS):
            pltpu.make_async_copy(wo_ref.at[:, columns(j)], wo_s.at[j], wo_sem.at[j]).start()
        for j in range(CUTS):
            pltpu.make_async_copy(x_ref.at[:, columns(j)], x_s.at[j], x_sem).start()

    def whole(s, slot, j):
        pltpu.make_async_copy(out_s.at[0, 0], out_s.at[0, 0], s.at[slot, j]).wait()

    def attended(s):
        starts = [pl.multiple_of(_ring(me, r, -(s + 1), side) * rows + r * part, part) for r in range(RINGS)]
        row = lax.broadcasted_iota(jnp.int32, (part, HEAD), 0)
        for r, at in enumerate(starts):
            place_s[r * part : (r + 1) * part, :] = row + at
            for h in range(heads):
                some_s[h, r * part : (r + 1) * part, :] = q_s[h, pl.ds(at, part), :]
        top_s[...] = jnp.full_like(top_s, NEG)
        total_s[...] = jnp.zeros_like(total_s)
        mix_s[...] = jnp.zeros_like(mix_s)

        def wide(t):
            return jnp.concatenate([t] * (KEYS // HEAD), axis=1)

        def block(c, _):
            pl.when(s == 0)(lambda: [copy.wait() for copy in given(c)] and None)
            here = pl.ds(pl.multiple_of(c * KEYS, KEYS), KEYS)
            hidden = lax.broadcasted_iota(jnp.int32, (rows, KEYS), 1) + c * KEYS > wide(place_s[...])
            scores = [_dot(some_s[h], k_s[h, here, :], 1, 1) for h in range(heads)]
            weights = []
            for h, t in enumerate(scores):
                t = jnp.where(hidden, HIDDEN, t)
                old = top_s[h]
                top = jnp.maximum(old, jnp.max(t, axis=1, keepdims=True))
                top_s[h] = top
                keep = jnp.exp2((old - top) * e)
                p = jnp.exp2((t - wide(top)) * e)
                total_s[h] = total_s[h] * keep + jnp.sum(p, axis=1, keepdims=True)
                weights.append((p.astype(jnp.bfloat16), keep))
            for h, (p, keep) in enumerate(weights):
                mix_s[h] = mix_s[h] * keep + _dot(p, v_s[h, here, :], 1, 0)
            pl.when((s == 0) & (c == 0))(fetch)

        last = lax.div(functools.reduce(jnp.maximum, starts) + part + KEYS - 1, KEYS)
        lax.fori_loop(0, last, block, None)

        def rest(c, _):
            for copy in given(c):
                copy.wait()

        pl.when(s == 0)(lambda: lax.fori_loop(last, blocks, rest, None))
        for h in range(heads):
            lhs_s[:, h * HEAD : (h + 1) * HEAD] = (mix_s[h] / total_s[h]).astype(jnp.bfloat16)

    def step(s, _):
        attended(s)
        slot, to, here = lax.rem(s, 2), lax.rem(s + 1, SLOTS), lax.rem(s, SLOTS)

        @pl.when((s >= SLOTS) & (s < n - 1))
        def _():
            for r in range(RINGS):
                pl.semaphore_wait(free_sem.at[r], 1)

        def cut(j, _):
            @pl.when(s == 0)
            def _():
                pltpu.make_async_copy(wo_s.at[j], wo_s.at[j], wo_sem.at[j]).wait()

            term_s[...] = _dot(lhs_s[...], wo_s[j], 1, 0)

            @pl.when(s >= 2)
            def _():
                whole(send_sem, slot, j)

            @pl.when(s == 0)
            def _():
                out_s[slot, j] = term_s[...].astype(jnp.bfloat16)

            @pl.when(s > 0)
            def _():
                whole(recv_sem, here, j)

            @pl.when((s > 0) & (s < n - 1))
            def _():
                out_s[slot, j] = (term_s[...] + in_s[here, j].astype(jnp.float32)).astype(jnp.bfloat16)

            @pl.when(s < n - 1)
            def _():
                for r in range(RINGS):
                    mine = pl.ds(r * part, part)
                    pltpu.make_async_remote_copy(src_ref=out_s.at[slot, j, mine, :], dst_ref=in_s.at[to, j, mine, :], send_sem=send_sem.at[slot, j],
                                                 recv_sem=recv_sem.at[to, j], device_id={"tp": ahead[r]}, device_id_type=MESH_ID).start()

            @pl.when(s == n - 1)
            def _():
                @pl.when(j == 0)
                def _():
                    pltpu.make_async_copy(x_s, x_s, x_sem).wait()

                sums = term_s[...] + in_s[here, j].astype(jnp.float32)
                y_ref[:, columns(j)] = (x_s[j].astype(jnp.float32) + sums).astype(jnp.bfloat16)

        lax.fori_loop(0, CUTS, cut, None)

        @pl.when((s > 0) & (s < n - SLOTS))
        def _():
            for r in range(RINGS):
                pl.semaphore_signal(free_sem.at[r], inc=1, device_id={"tp": ahead[r ^ 1]}, device_id_type=MESH_ID)

    lax.fori_loop(0, n, step, None)
    for j in range(CUTS):
        whole(send_sem, (n - 2) % 2, j)


def attend_project_scatter(q, k, v, wo, x, n):
    rows, depth = x.shape
    heads = q.shape[0]
    state = pltpu.VMEM((heads, rows, HEAD), jnp.float32)
    hbm = pl.BlockSpec(memory_space=pltpu.HBM)
    dma = pltpu.SemaphoreType.DMA
    width = depth // CUTS
    return pl.pallas_call(
        functools.partial(_scatter_kernel, n),
        out_shape=pltpu.VMEM((rows, depth), jnp.bfloat16),
        in_specs=[hbm] * 5,
        out_specs=pl.BlockSpec(memory_space=pltpu.VMEM),
        scratch_shapes=[
            pltpu.VMEM((CUTS, heads * HEAD, width), jnp.bfloat16),
            *[pltpu.VMEM(q.shape, jnp.bfloat16)] * 3,
            pltpu.VMEM((SLOTS, CUTS, rows, width), jnp.bfloat16),
            pltpu.VMEM((2, CUTS, rows, width), jnp.bfloat16),
            pltpu.VMEM((rows, heads * HEAD), jnp.bfloat16),
            pltpu.VMEM((rows, width), jnp.float32),
            pltpu.VMEM((CUTS, rows, width), jnp.bfloat16),
            pltpu.VMEM((heads, rows, HEAD), jnp.bfloat16), state, state, state,
            pltpu.VMEM((rows, HEAD), jnp.int32),
            dma(()), dma((2, n * rows // KEYS)), dma((CUTS,)), dma(()), dma((2, CUTS)), dma((SLOTS, CUTS)), pltpu.SemaphoreType.REGULAR((RINGS,)),
        ],
        compiler_params=pltpu.CompilerParams(collective_id=1, has_side_effects=True, vmem_limit_bytes=59 * 2**20),
        cost_estimate=pl.CostEstimate(flops=2 * n * rows * depth * heads * HEAD, bytes_accessed=4 * n * rows * depth, transcendentals=0),
        name="attend_project_scatter",
    )(q, k, v, wo, x)


def _turns(rows):
    half = HEAD // 2
    angle = np.arange(rows, dtype=np.float32)[:, None] * np.float32(THETA) ** (-np.arange(half, dtype=np.float32) / np.float32(half))
    return np.concatenate([np.cos(angle), np.sin(angle)], -1).astype(np.float32)


def solution(mesh):
    n = mesh.shape["tp"]

    def step(x, gain, wq, wk, wv, wo):
        _, q, k, v = gather_project(x, gain, jnp.asarray(_turns(n * x.shape[0])), wq, wk, wv, n)
        return attend_project_scatter(q, k, v, wo, x, n)

    tokens, columns = P(("dp", "tp"), None), P(None, "tp")
    return jax.shard_map(
        step,
        mesh=mesh,
        in_specs=(tokens, P(None), columns, columns, columns, P("tp", None)),
        out_specs=tokens,
        check_vma=False,
    )
```
